32 devices in a mesh: leaf: 16 (over z, y, x), tile: 2 (over core).
Axes of the slice: x: 2, y: 2, z: 4, core: 2. Of those that a mesh axis runs over, the one named last changes fastest.
Arguments:
- rhs: float32 [5, 64, 8, 128], P(None, ('leaf', 'tile')), may hold values from -6 to 6
- lower: bfloat16 [4, 64, 3, 128, 128], P(None, ('leaf', 'tile')), may hold values from -0.21875 to 0.21875
- upper: bfloat16 [4, 64, 3, 128, 128], P(None, ('leaf', 'tile')), may hold values from -0.21875 to 0.21875
- diag_inv: bfloat16 [5, 64, 128, 128], P(None, ('leaf', 'tile')), may hold values from -0.4 to 1.4
- pattern: int32 [4, 64, 3], replicated, may hold values from 0 to 63, as said below
- counts: int32 [5, 32], P(None, ('leaf', 'tile')), may hold values from 1 to 2
- basis: float32 [8, 5, 64, 8, 128], P(None, None, ('leaf', 'tile')), may hold values from -1 to 1, as said below
Outputs:
- precond: float32 [5, 64, 8, 128], P(None, ('leaf', 'tile'))
- coeffs: float32 [9, 8], replicated
The draws below stay inside these ranges and needn't reach their ends.
Inputs may be any that keep to these rules, and one draw needn't show every extreme that they name: `pattern`: the entries of level index i (connector level i + 1) lie below 2 ** (i + 2) * 2: tiles of the level below within the same group, numbered device by device and slot by slot. `counts`: slots 0 to count - 1 of a device at a level hold tiles; the other slots are empty. `basis`: for each right-hand side the 8 vectors are orthonormal over all unknowns.
All inputs are finite; a program needn't handle non-finite values.
Results may differ from the reference program's by a relative error of at most 0.009.
Values may be sent and summed in bfloat16 or wider, within the bound.
A program may use at most 64 MiB of HBM per device.

```python
import math
import jax
import jax.numpy as jnp
import numpy as np
from jax import lax

TILE_ROWS = 128
RHS = 8
TILES_DEV = 2
NEIGHBOURS = 3
BASIS = 8
LEVELS = 5
TILES = 64
N_LEAF = 16
N_TILE = 2


def draw_diag_inv(key, part):
    half_width = min(0.35, 0.5 * math.sqrt(3.0 / TILE_ROWS))
    noise = jax.random.uniform(key, (LEVELS, TILES, TILE_ROWS, TILE_ROWS), jnp.float32, -half_width, half_width)
    return (noise + jnp.eye(TILE_ROWS, dtype=jnp.float32)).astype(jnp.bfloat16)


def draw_pattern(key, part):
    ceiling = np.array([2 ** (level + 2) * TILES_DEV for level in range(LEVELS - 1)], dtype=np.int32)
    return jax.random.randint(key, (LEVELS - 1, TILES, NEIGHBOURS), 0, jnp.asarray(ceiling)[:, None, None], dtype=jnp.int32)


def draw_basis(key, part):
    samples = jax.random.normal(key, (RHS, BASIS, LEVELS * TILES * TILE_ROWS), jnp.float32)
    vectors = []
    for column in range(BASIS):
        vector = samples[:, column]
        for repeat in range(2):
            for earlier in vectors:
                vector = vector - jnp.sum(vector * earlier, -1, keepdims=True) * earlier
        vector = vector / jnp.sqrt(jnp.sum(vector * vector, -1, keepdims=True))
        vectors.append(vector)
    stacked = jnp.stack(vectors, 0).reshape(BASIS, RHS, LEVELS, TILES, TILE_ROWS)
    return jnp.transpose(stacked, (0, 2, 3, 1, 4))


def place_ends(result, stream_key, smallest, top_value):
    place = [jax.random.randint(jax.random.fold_in(stream_key, axis), (), 0, length) for axis, length in enumerate(result.shape)]
    widest = result.shape.index(max(result.shape))
    neighbour = place[:widest] + [(place[widest] + 1) % result.shape[widest]] + place[widest + 1:]
    return result.at[tuple(place)].set(smallest).at[tuple(neighbour)].set(top_value)


def steps_of(rng, shape, split, least, high):
    factor_of, own = 1.0, jax.random.fold_in(rng, 6)
    for dim, blocks in split:
        steps = jnp.exp(jax.random.uniform(jax.random.fold_in(own, dim), (blocks,), jnp.float32, least / len(split), high / len(split)))
        factor_of = factor_of * jnp.repeat(steps, shape[dim] // blocks).reshape([-1 if axis == dim else 1 for axis in range(len(shape))])
    return factor_of


def scatter_about(rng, shape, scale, bound, pieces=(), held_as=jnp.bfloat16):
    values = scale * jax.random.normal(rng, shape, jnp.float32)
    if pieces:
        values = values * steps_of(rng, shape, pieces, -0.22, 0.18)
    return jnp.clip(values, -bound, bound).astype(held_as)


def setup_inputs(seed: int = 0) -> dict:
    keys = jax.random.split(jax.random.key(seed), 8)
    rhs = scatter_about(keys[0], (LEVELS, TILES, RHS, TILE_ROWS), 1.0, 6.0, ((1, 32),), jnp.float32)
    lower = scatter_about(keys[1], (LEVELS - 1, TILES, NEIGHBOURS, TILE_ROWS, TILE_ROWS), (2 * NEIGHBOURS * TILE_ROWS) ** -0.5, 0.21875, ((1, 32),))
    upper = scatter_about(keys[2], (LEVELS - 1, TILES, NEIGHBOURS, TILE_ROWS, TILE_ROWS), (2 * NEIGHBOURS * TILE_ROWS) ** -0.5, 0.21875, ((1, 32),))
    diag_inv = draw_diag_inv(jax.random.fold_in(keys[7], 71), 0)
    pattern = draw_pattern(jax.random.fold_in(keys[7], 71), 0)
    counts = place_ends(jax.random.randint(keys[5], (LEVELS, N_LEAF * N_TILE), 1, TILES_DEV + 1), jax.random.fold_in(keys[5], 1), 1, TILES_DEV).astype(jnp.int32)
    basis = draw_basis(jax.random.fold_in(keys[7], 71), 0)
    return {"rhs": rhs, "lower": lower, "upper": upper, "diag_inv": diag_inv, "pattern": pattern, "counts": counts, "basis": basis}


epsilon = 1e-06

def reference(rhs, lower, upper, diag_inv, pattern, counts, basis):
    tile_total = TILES
    slot_index = jnp.arange(tile_total, dtype=jnp.int32) % TILES_DEV
    owner_device = jnp.arange(tile_total, dtype=jnp.int32) // TILES_DEV
    live_mask = (slot_index[None, :] < counts[:, owner_device]).astype(jnp.float32)[:, :, None, None]

    def sources(level_index):
        span = 2 ** (level_index + 1)
        group_start = owner_device // span * span * TILES_DEV
        return (group_start[:, None] + pattern[level_index - 1]).astype(jnp.int32)
    forward_vals = [live_mask[0] * rhs[0]]
    for level_index in range(1, LEVELS):
        previous = lax.optimization_barrier(forward_vals[-1].astype(jnp.bfloat16)).astype(jnp.float32)
        picked = previous[sources(level_index)]
        coupling = jnp.einsum('tnab,tnrb->tra', lower[level_index - 1].astype(jnp.float32), picked)
        forward_vals.append(live_mask[level_index] * (rhs[level_index] - coupling))
    solutions = [None] * LEVELS
    upstream = jnp.zeros_like(rhs[0])
    for level_index in reversed(range(LEVELS)):
        operand = lax.optimization_barrier((forward_vals[level_index] - upstream).astype(jnp.bfloat16)).astype(jnp.float32)
        solution = live_mask[level_index] * jnp.einsum('tab,trb->tra', diag_inv[level_index].astype(jnp.float32), operand)
        solutions[level_index] = solution
        if level_index > 0:
            rounded = lax.optimization_barrier(solution.astype(jnp.bfloat16)).astype(jnp.float32)
            products = jnp.einsum('tnab,trb->tnra', upper[level_index - 1].astype(jnp.float32), rounded)
            flat = products.reshape(tile_total * NEIGHBOURS, RHS, TILE_ROWS)
            upstream = jax.ops.segment_sum(flat, sources(level_index).reshape(-1), num_segments=tile_total)
    precond = jnp.stack(solutions, 0)
    projections = jnp.einsum('mltrb,ltrb->mr', basis, precond, precision=lax.Precision.HIGHEST)
    remainder = precond - jnp.einsum('mr,mltrb->ltrb', projections, basis, precision=lax.Precision.HIGHEST)
    length_norm = jnp.sqrt(lax.optimization_barrier(jnp.sum(remainder * remainder, axis=(0, 1, 3))) + epsilon)
    scaled = length_norm / jnp.sqrt(jnp.float32(LEVELS * tile_total * TILE_ROWS))
    coeffs = jnp.concatenate([projections, scaled[None, :]], 0)
    return (precond, coeffs)
```

```python
import functools
import math

import jax
import jax.numpy as jnp
from jax import lax
from jax.experimental import pallas as pl
from jax.experimental.pallas import tpu as pltpu
from jax.sharding import PartitionSpec as P

epsilon = 1e-06
MESH = pl.DeviceIdType.MESH
NT = (((1,), (1,)), ((), ()))


def split(index, size):
    if size & (size - 1) == 0:
        return lax.shift_right_logical(index, size.bit_length() - 1), index & (size - 1)
    return index // size, index % size


def kernel(dims, *refs):
    levels, tiles, columns, rows, neighbours, basis_size, n_leaf, n_tile = dims
    devices = n_leaf * n_tile
    width = tiles * columns
    pairs = tiles * neighbours
    refs = list(refs)

    def take(count):
        taken = refs[:count]
        del refs[:count]
        return taken

    rhs_any, lower_any, upper_any, diag_any, pattern_any, counts_any, basis_any = take(7)
    precond_ref, coeffs_ref = take(2)
    rhs_v, lower_v, upper_v, diag_v, pattern_v, counts_v, basis_v = take(7)
    gathered = take(levels - 1)
    outgoing = take(levels - 1)
    incoming = take(levels - 1)
    pick = take(levels - 1)
    spread = take(levels - 1)
    (totals,) = take(1)
    load_sem, fwd_send, fwd_recv, bwd_send, bwd_recv, sum_send, sum_recv = take(7)

    leaf = lax.axis_index("leaf")
    tile = lax.axis_index("tile")
    me = leaf * n_tile + tile

    def load(number, source, target):
        copy = pltpu.make_async_copy(source, target, load_sem.at[number])
        copy.start()
        return copy

    rhs_load = load(0, rhs_any, rhs_v)
    pattern_load = load(1, pattern_any, pattern_v)
    counts_load = load(2, counts_any, counts_v)
    lower_load = [
        load(3 + k, lower_any.at[k], lower_v.at[k]) for k in range(levels - 1)
    ]
    diag_load = load(levels + 2, diag_any, diag_v)
    upper_load = load(levels + 3, upper_any, upper_v)
    basis_load = load(levels + 4, basis_any, basis_v)

    def each_peer(leaves, visit):
        first = lax.div(leaf, leaves) * leaves
        own = leaf - first
        others = [(tile + step) % n_tile if step else tile for step in range(n_tile)]

        def far(step, carry):
            near = lax.rem(own + step, leaves)
            for other in others:
                visit(first + near, other, near * n_tile + other)
            return carry

        if leaves <= 16:
            for step in range(leaves // 2, leaves):
                far(step, 0)
            for step in range(1, leaves // 2):
                far(step, 0)
        else:
            lax.fori_loop(1, leaves, far, 0)
        for other in others[1:]:
            visit(leaf, other, own * n_tile + other)

    barrier = pltpu.get_barrier_semaphore()

    def greet(to_leaf, to_tile, index):
        pl.semaphore_signal(barrier, inc=1, device_id=(to_leaf, to_tile), device_id_type=MESH)

    each_peer(n_leaf, greet)

    rhs_load.wait()
    pattern_load.wait()
    counts_load.wait()
    live = [
        [
            (counts_v[k : k + 1, 0:1] > t).astype(jnp.float32)
            for t in range(tiles)
        ]
        for k in range(levels)
    ]

    def selectors(k):
        span = gathered[k].shape[0]
        table = pattern_v[k]
        row = lax.broadcasted_iota(jnp.int32, table.shape, 0)
        numbers = []
        for t in range(tiles):
            mine = jnp.sum(
                jnp.where(row == me * tiles + t, table, 0), axis=0, keepdims=True
            )
            numbers += [mine[:, n : n + 1] for n in range(neighbours)]
        lane_tile, lane_column = split(
            lax.broadcasted_iota(jnp.int32, (columns, span * width), 1), columns
        )
        same = lane_column == lax.broadcasted_iota(jnp.int32, (columns, span * width), 0)
        blocks = [
            jnp.where(same & (lane_tile == number), 1.0, 0.0) for number in numbers
        ]
        pick[k][...] = jnp.concatenate(blocks, 0).astype(jnp.bfloat16)
        lane_pair, lane_column = split(
            lax.broadcasted_iota(jnp.int32, (1, pairs * columns), 1), columns
        )
        wanted = jnp.zeros((1, pairs * columns), jnp.int32)
        for q, number in enumerate(numbers):
            wanted = jnp.where(lane_pair == q, number, wanted)
        row_tile, row_column = split(
            lax.broadcasted_iota(jnp.int32, (span * width, pairs * columns), 0), columns
        )
        chosen = (row_tile == wanted) & (row_column == lane_column)
        spread[k][...] = jnp.where(chosen, 1.0, 0.0).astype(jnp.bfloat16)

    selectors(0)

    def group(k):
        span = gathered[k].shape[0]
        return span, lax.rem(me, span)

    def arrived(buffer, semaphore, span):
        part = buffer.at[pl.ds(0, span - 1)]
        pltpu.make_async_copy(part, part, semaphore).wait()

    forward_vals = [[live[0][t] * rhs_v[0, t] for t in range(tiles)]]
    for k in range(1, levels):
        buffer = gathered[k - 1]
        span, slot = group(k - 1)
        buffer[slot] = jnp.concatenate(forward_vals[-1], 0).astype(jnp.bfloat16)
        if k == 1:
            pl.semaphore_wait(barrier, devices - 1)

        def send(to_leaf, to_tile, index):
            pltpu.make_async_remote_copy(
                src_ref=buffer.at[slot],
                dst_ref=buffer.at[slot],
                send_sem=fwd_send.at[k - 1],
                recv_sem=fwd_recv.at[k - 1],
                device_id=(to_leaf, to_tile),
                device_id_type=MESH,
            ).start()

        each_peer(span // n_tile, send)
        if k < levels - 1:
            selectors(k)
        lower_load[k - 1].wait()
        arrived(buffer, fwd_recv.at[k - 1], span)
        picked = jnp.dot(
            pick[k - 1][...],
            buffer[...].reshape(span * width, rows),
            preferred_element_type=jnp.float32,
        ).astype(jnp.bfloat16)
        values = []
        for t in range(tiles):
            coupling = None
            for n in range(neighbours):
                q = t * neighbours + n
                term = lax.dot_general(
                    picked[q * columns : (q + 1) * columns],
                    lower_v[k - 1, t, n],
                    NT,
                    preferred_element_type=jnp.float32,
                )
                coupling = term if coupling is None else coupling + term
            values.append(live[k][t] * (rhs_v[k, t] - coupling))
        forward_vals.append(values)

    diag_load.wait()
    upper_load.wait()
    basis_load.wait()
    partial = [None] * basis_size
    squares = None

    def project(k, values):
        nonlocal squares
        for t in range(tiles):
            for m in range(basis_size):
                term = basis_v[m, k, t] * values[t]
                partial[m] = term if partial[m] is None else partial[m] + term
            term = values[t] * values[t]
            squares = term if squares is None else squares + term

    upstream = None
    for k in reversed(range(levels)):
        values = []
        for t in range(tiles):
            operand = forward_vals[k][t]
            if upstream is not None:
                operand = operand - upstream[t * columns : (t + 1) * columns]
            value = live[k][t] * lax.dot_general(
                operand.astype(jnp.bfloat16),
                diag_v[k, t],
                NT,
                preferred_element_type=jnp.float32,
            )
            precond_ref[k, t] = value
            values.append(value)
        if k > 0:
            span, slot = group(k - 1)
            products = []
            for t in range(tiles):
                rounded = values[t].astype(jnp.bfloat16)
                for n in range(neighbours):
                    products.append(
                        lax.dot_general(
                            rounded,
                            upper_v[k - 1, t, n],
                            NT,
                            preferred_element_type=jnp.float32,
                        )
                    )
            products = jnp.concatenate(products, 0).astype(jnp.bfloat16)
            out, into = outgoing[k - 1], incoming[k - 1]
            out[...] = (
                jnp.dot(spread[k - 1][...], products, preferred_element_type=jnp.float32)
                .astype(jnp.bfloat16)
                .reshape(span, width, rows)
            )

            def send(to_leaf, to_tile, index):
                pltpu.make_async_remote_copy(
                    src_ref=out.at[index],
                    dst_ref=into.at[slot],
                    send_sem=bwd_send.at[k - 1],
                    recv_sem=bwd_recv.at[k - 1],
                    device_id=(to_leaf, to_tile),
                    device_id_type=MESH,
                ).start()

            each_peer(span // n_tile, send)
            into[slot] = out[slot]
            project(k, values)
            arrived(into, bwd_recv.at[k - 1], span)
            upstream = jnp.sum(into[...].astype(jnp.float32), axis=0)
        else:
            project(k, values)

    lane = lax.broadcasted_iota(jnp.int32, (columns, rows), 1)
    packed = jnp.zeros((columns, rows), jnp.float32)
    for m, term in enumerate(partial + [squares]):
        packed = jnp.where(lane == m, jnp.sum(term, axis=1, keepdims=True), packed)
    totals[me] = packed

    def send(to_leaf, to_tile, index):
        pltpu.make_async_remote_copy(
            src_ref=totals.at[me],
            dst_ref=totals.at[me],
            send_sem=sum_send,
            recv_sem=sum_recv,
            device_id=(to_leaf, to_tile),
            device_id_type=MESH,
        ).start()

    each_peer(n_leaf, send)
    for k in range(1, levels):
        span, slot = group(k - 1)
        arrived(gathered[k - 1], fwd_send.at[k - 1], span)
        arrived(outgoing[k - 1], bwd_send.at[k - 1], span)
    arrived(totals, sum_recv, devices)
    total = jnp.sum(totals[...], axis=0)
    squared = jnp.sum(jnp.where(lane == basis_size, total, 0.0), axis=1, keepdims=True)
    explained = jnp.sum(
        jnp.where(lane < basis_size, total * total, 0.0), axis=1, keepdims=True
    )
    norm = jnp.sqrt(jnp.maximum(squared - explained, 0.0) + epsilon)
    scaled = norm / math.sqrt(levels * tiles * rows * devices)
    result = jnp.where(lane == basis_size, scaled, total)
    coeffs_ref[...] = jnp.transpose(result)[: basis_size + 1]
    arrived(totals, sum_send, devices)


def local(rhs, lower, upper, diag_inv, pattern, counts, basis):
    levels, tiles, columns, rows = rhs.shape
    neighbours = lower.shape[2]
    basis_size = basis.shape[0]
    n_leaf, n_tile = lax.axis_size("leaf"), lax.axis_size("tile")
    dims = (levels, tiles, columns, rows, neighbours, basis_size, n_leaf, n_tile)
    spans = [2 ** (k + 1) for k in range(1, levels)]
    width, pairs = tiles * columns, tiles * neighbours
    operands = (rhs, lower, upper, diag_inv, pattern, counts, basis)
    slots = [pltpu.VMEM((span, width, rows), jnp.bfloat16) for span in spans]
    scratch = [pltpu.VMEM(operand.shape, operand.dtype) for operand in operands]
    scratch += slots * 3
    scratch += [pltpu.VMEM((pairs * columns, span * width), jnp.bfloat16) for span in spans]
    scratch += [pltpu.VMEM((span * width, pairs * columns), jnp.bfloat16) for span in spans]
    scratch += [pltpu.VMEM((n_leaf * n_tile, columns, rows), jnp.float32)]
    scratch += [pltpu.SemaphoreType.DMA((levels + 5,))]
    scratch += [pltpu.SemaphoreType.DMA((levels - 1,))] * 4
    scratch += [pltpu.SemaphoreType.DMA] * 2
    return pl.pallas_call(
        functools.partial(kernel, dims),
        name="sweep",
        out_shape=(
            jax.ShapeDtypeStruct(rhs.shape, jnp.float32),
            jax.ShapeDtypeStruct((basis_size + 1, columns), jnp.float32),
        ),
        in_specs=[pl.BlockSpec(memory_space=pl.ANY)] * len(operands),
        out_specs=[pl.BlockSpec(memory_space=pltpu.VMEM)] * 2,
        scratch_shapes=scratch,
        compiler_params=pltpu.CompilerParams(collective_id=0, has_side_effects=True),
    )(*operands)


def solution(mesh):
    return jax.shard_map(
        local,
        mesh=mesh,
        in_specs=(
            P(None, ("leaf", "tile"), None, None),
            P(None, ("leaf", "tile"), None, None, None),
            P(None, ("leaf", "tile"), None, None, None),
            P(None, ("leaf", "tile"), None, None),
            P(),
            P(None, ("leaf", "tile")),
            P(None, None, ("leaf", "tile"), None, None),
        ),
        out_specs=(P(None, ("leaf", "tile"), None, None), P()),
        check_vma=False,
    )
```

```python
import functools
import math

import jax
import jax.numpy as jnp
from jax import lax
from jax.experimental import pallas as pl
from jax.experimental.pallas import tpu as pltpu
from jax.sharding import PartitionSpec as P

epsilon = 1e-06
MESH = pl.DeviceIdType.MESH
NT = (((1,), (1,)), ((), ()))


def split(index, size):
    if size & (size - 1) == 0:
        return lax.shift_right_logical(index, size.bit_length() - 1), index & (size - 1)
    return index // size, index % size


def kernel(dims, *refs):
    levels, tiles, columns, rows, neighbours, basis_size, n_leaf, n_tile = dims
    devices = n_leaf * n_tile
    width = tiles * columns
    pairs = tiles * neighbours
    refs = list(refs)

    def take(count):
        taken = refs[:count]
        del refs[:count]
        return taken

    rhs_any, lower_any, upper_any, diag_any, pattern_any, counts_any, basis_any = take(7)
    precond_ref, coeffs_ref = take(2)
    rhs_v, lower_v, upper_v, diag_v, counts_v, basis_v = take(6)
    gathered = take(levels - 1)
    outgoing = take(levels - 1)
    incoming = take(levels - 1)
    (pattern_s,) = take(1)
    spread = take(levels - 1)
    (totals,) = take(1)
    load_sem, fwd_send, fwd_recv, bwd_send, bwd_recv, sum_send, sum_recv = take(7)

    leaf = lax.axis_index("leaf")
    tile = lax.axis_index("tile")
    me = leaf * n_tile + tile

    def load(number, source, target):
        copy = pltpu.make_async_copy(source, target, load_sem.at[number])
        copy.start()
        return copy

    rhs_load = load(0, rhs_any, rhs_v)
    pattern_load = load(1, pattern_any, pattern_s)
    counts_load = load(2, counts_any, counts_v)
    lower_load = [
        load(3 + k, lower_any.at[k], lower_v.at[k]) for k in range(levels - 1)
    ]
    diag_load = load(levels + 2, diag_any, diag_v)
    upper_load = load(levels + 3, upper_any, upper_v)
    basis_load = load(levels + 4, basis_any, basis_v)

    def each_peer(leaves, visit):
        first = lax.div(leaf, leaves) * leaves
        own = leaf - first
        others = [(tile + step) % n_tile if step else tile for step in range(n_tile)]

        def far(step, carry):
            near = lax.rem(own + step, leaves)
            for other in others:
                visit(first + near, other, near * n_tile + other)
            return carry

        if leaves <= 16:
            for step in range(leaves // 2, leaves):
                far(step, 0)
            for step in range(1, leaves // 2):
                far(step, 0)
        else:
            lax.fori_loop(1, leaves, far, 0)
        for other in others[1:]:
            visit(leaf, other, own * n_tile + other)

    barrier = pltpu.get_barrier_semaphore()

    def greet(to_leaf, to_tile, index):
        pl.semaphore_signal(barrier, inc=1, device_id=(to_leaf, to_tile), device_id_type=MESH)

    each_peer(n_leaf, greet)

    rhs_load.wait()
    pattern_load.wait()
    counts_load.wait()
    live = [
        [
            (counts_v[0:1, k : k + 1] > t).astype(jnp.float32)
            for t in range(tiles)
        ]
        for k in range(levels)
    ]

    def source(k, t, n):
        return pattern_s[n, k, me * tiles + t]

    def selectors(k):
        span = gathered[k].shape[0]
        lane_pair, lane_column = split(
            lax.broadcasted_iota(jnp.int32, (1, pairs * columns), 1), columns
        )
        wanted = jnp.zeros((1, pairs * columns), jnp.int32)
        for t in range(tiles):
            for n in range(neighbours):
                wanted = jnp.where(lane_pair == t * neighbours + n, source(k, t, n), wanted)
        row_tile, row_column = split(
            lax.broadcasted_iota(jnp.int32, (span * width, pairs * columns), 0), columns
        )
        chosen = (row_tile == wanted) & (row_column == lane_column)
        spread[k][...] = jnp.where(chosen, 1.0, 0.0).astype(jnp.bfloat16)

    selectors(0)

    def group(k):
        span = gathered[k].shape[0]
        return span, lax.rem(me, span)

    def arrived(buffer, semaphore, span):
        part = buffer.at[pl.ds(0, span - 1)]
        pltpu.make_async_copy(part, part, semaphore).wait()

    forward_vals = [[live[0][t] * rhs_v[0, t] for t in range(tiles)]]
    for k in range(1, levels):
        buffer = gathered[k - 1]
        span, slot = group(k - 1)
        buffer[slot] = jnp.concatenate(forward_vals[-1], 0).astype(jnp.bfloat16)
        if k == 1:
            pl.semaphore_wait(barrier, devices - 1)

        def send(to_leaf, to_tile, index):
            pltpu.make_async_remote_copy(
                src_ref=buffer.at[slot],
                dst_ref=buffer.at[slot],
                send_sem=fwd_send.at[k - 1],
                recv_sem=fwd_recv.at[k - 1],
                device_id=(to_leaf, to_tile),
                device_id_type=MESH,
            ).start()

        each_peer(span // n_tile, send)
        if k < levels - 1:
            selectors(k)
        lower_load[k - 1].wait()
        arrived(buffer, fwd_recv.at[k - 1], span)
        picked = []
        for t in range(tiles):
            for n in range(neighbours):
                owner, place = split(source(k - 1, t, n), tiles)
                both = buffer[owner].astype(jnp.float32)
                chosen = both[:columns]
                for other in range(1, tiles):
                    part = both[other * columns : (other + 1) * columns]
                    chosen = jnp.where(place == other, part, chosen)
                picked.append(chosen.astype(jnp.bfloat16))
        values = []
        for t in range(tiles):
            coupling = None
            for n in range(neighbours):
                q = t * neighbours + n
                term = lax.dot_general(
                    picked[q],
                    lower_v[k - 1, t, n],
                    NT,
                    preferred_element_type=jnp.float32,
                )
                coupling = term if coupling is None else coupling + term
            values.append(live[k][t] * (rhs_v[k, t] - coupling))
        forward_vals.append(values)

    diag_load.wait()
    upper_load.wait()
    basis_load.wait()
    partial = [None] * basis_size
    squares = None

    def project(k, values):
        nonlocal squares
        for t in range(tiles):
            for m in range(basis_size):
                term = basis_v[m, k, t] * values[t]
                partial[m] = term if partial[m] is None else partial[m] + term
            term = values[t] * values[t]
            squares = term if squares is None else squares + term

    upstream = None
    for k in reversed(range(levels)):
        values = []
        for t in range(tiles):
            operand = forward_vals[k][t]
            if upstream is not None:
                operand = operand - upstream[t * columns : (t + 1) * columns]
            value = live[k][t] * lax.dot_general(
                operand.astype(jnp.bfloat16),
                diag_v[k, t],
                NT,
                preferred_element_type=jnp.float32,
            )
            precond_ref[k, t] = value
            values.append(value)
        if k > 0:
            span, slot = group(k - 1)
            products = []
            for t in range(tiles):
                rounded = values[t].astype(jnp.bfloat16)
                for n in range(neighbours):
                    products.append(
                        lax.dot_general(
                            rounded,
                            upper_v[k - 1, t, n],
                            NT,
                            preferred_element_type=jnp.float32,
                        )
                    )
            products = jnp.concatenate(products, 0).astype(jnp.bfloat16)
            out, into = outgoing[k - 1], incoming[k - 1]
            out[...] = (
                jnp.dot(spread[k - 1][...], products, preferred_element_type=jnp.float32)
                .astype(jnp.bfloat16)
                .reshape(span, width, rows)
            )

            def send(to_leaf, to_tile, index):
                pltpu.make_async_remote_copy(
                    src_ref=out.at[index],
                    dst_ref=into.at[slot],
                    send_sem=bwd_send.at[k - 1],
                    recv_sem=bwd_recv.at[k - 1],
                    device_id=(to_leaf, to_tile),
                    device_id_type=MESH,
                ).start()

            each_peer(span // n_tile, send)
            into[slot] = out[slot]
            project(k, values)
            arrived(into, bwd_recv.at[k - 1], span)
            upstream = jnp.sum(into[...].astype(jnp.float32), axis=0)
        else:
            project(k, values)

    lane = lax.broadcasted_iota(jnp.int32, (columns, rows), 1)
    seat = lane - lax.broadcasted_iota(jnp.int32, (columns, rows), 0)
    packed = jnp.zeros((columns, rows), jnp.float32)
    for m, term in enumerate(partial + [squares]):
        reduced = jnp.sum(term, axis=1, keepdims=True)
        packed = jnp.where(seat == m * columns, reduced, packed)
    totals[me] = jnp.sum(packed, axis=0, keepdims=True)

    def send(to_leaf, to_tile, index):
        pltpu.make_async_remote_copy(
            src_ref=totals.at[me],
            dst_ref=totals.at[me],
            send_sem=sum_send,
            recv_sem=sum_recv,
            device_id=(to_leaf, to_tile),
            device_id_type=MESH,
        ).start()

    each_peer(n_leaf, send)
    for k in range(1, levels):
        span, slot = group(k - 1)
        arrived(gathered[k - 1], fwd_send.at[k - 1], span)
        arrived(outgoing[k - 1], bwd_send.at[k - 1], span)
    arrived(totals, sum_recv, devices)
    summed = jnp.broadcast_to(jnp.sum(totals[...], axis=0), (columns, rows))
    spaced = jnp.where(split(lane, columns)[1] == lane - seat, summed, 0.0)
    row_block, _ = split(lax.broadcasted_iota(jnp.int32, (rows, rows), 0), columns)
    compress = row_block == lax.broadcasted_iota(jnp.int32, (rows, rows), 1)
    total = jnp.dot(
        spaced,
        jnp.where(compress, 1.0, 0.0),
        precision=lax.Precision.HIGHEST,
        preferred_element_type=jnp.float32,
    )
    squared = jnp.sum(jnp.where(lane == basis_size, total, 0.0), axis=1, keepdims=True)
    explained = jnp.sum(
        jnp.where(lane < basis_size, total * total, 0.0), axis=1, keepdims=True
    )
    norm = jnp.sqrt(jnp.maximum(squared - explained, 0.0) + epsilon)
    scaled = norm / math.sqrt(levels * tiles * rows * devices)
    result = jnp.where(lane == basis_size, scaled, total)
    coeffs_ref[...] = result[:, : basis_size + 1]
    arrived(totals, sum_send, devices)


def local(rhs, lower, upper, diag_inv, pattern, counts, basis):
    levels, tiles, columns, rows = rhs.shape
    neighbours = lower.shape[2]
    basis_size = basis.shape[0]
    n_leaf, n_tile = lax.axis_size("leaf"), lax.axis_size("tile")
    dims = (levels, tiles, columns, rows, neighbours, basis_size, n_leaf, n_tile)
    spans = [2 ** (k + 1) for k in range(1, levels)]
    width, pairs = tiles * columns, tiles * neighbours
    pattern, counts = jnp.transpose(pattern, (2, 0, 1)), counts.T
    operands = (rhs, lower, upper, diag_inv, pattern, counts, basis)
    slots = [pltpu.VMEM((span, width, rows), jnp.bfloat16) for span in spans]
    scratch = [
        pltpu.VMEM(operand.shape, operand.dtype) for operand in operands if operand is not pattern
    ]
    scratch += slots * 3
    scratch += [pltpu.SMEM(pattern.shape, pattern.dtype)]
    scratch += [pltpu.VMEM((span * width, pairs * columns), jnp.bfloat16) for span in spans]
    scratch += [pltpu.VMEM((n_leaf * n_tile, 1, rows), jnp.float32)]
    scratch += [pltpu.SemaphoreType.DMA((levels + 5,))]
    scratch += [pltpu.SemaphoreType.DMA((levels - 1,))] * 4
    scratch += [pltpu.SemaphoreType.DMA] * 2
    precond, coeffs = pl.pallas_call(
        functools.partial(kernel, dims),
        name="sweep",
        out_shape=(
            jax.ShapeDtypeStruct(rhs.shape, jnp.float32),
            jax.ShapeDtypeStruct((columns, basis_size + 1), jnp.float32),
        ),
        in_specs=[pl.BlockSpec(memory_space=pl.ANY)] * len(operands),
        out_specs=[pl.BlockSpec(memory_space=pltpu.VMEM)] * 2,
        scratch_shapes=scratch,
        compiler_params=pltpu.CompilerParams(collective_id=0, has_side_effects=True),
    )(*operands)
    return precond, coeffs.T


def solution(mesh):
    return jax.shard_map(
        local,
        mesh=mesh,
        in_specs=(
            P(None, ("leaf", "tile"), None, None),
            P(None, ("leaf", "tile"), None, None, None),
            P(None, ("leaf", "tile"), None, None, None),
            P(None, ("leaf", "tile"), None, None),
            P(),
            P(None, ("leaf", "tile")),
            P(None, None, ("leaf", "tile"), None, None),
        ),
        out_specs=(P(None, ("leaf", "tile"), None, None), P()),
        check_vma=False,
    )
```

```python
import functools
import math

import jax
import jax.numpy as jnp
from jax import lax
from jax.experimental import pallas as pl
from jax.experimental.pallas import tpu as pltpu
from jax.sharding import PartitionSpec as P

epsilon = 1e-06
MESH = pl.DeviceIdType.MESH
NT = (((1,), (1,)), ((), ()))


def split(index, size):
    if size & (size - 1) == 0:
        return lax.shift_right_logical(index, size.bit_length() - 1), index & (size - 1)
    return index // size, index % size


def kernel(dims, *refs):
    levels, tiles, columns, rows, neighbours, basis_size, n_leaf, n_tile = dims
    devices = n_leaf * n_tile
    width = tiles * columns
    pairs = tiles * neighbours
    refs = list(refs)

    def take(count):
        taken = refs[:count]
        del refs[:count]
        return taken

    rhs_any, lower_any, upper_any, diag_any, pattern_any, counts_any, basis_any = take(7)
    precond_ref, coeffs_ref = take(2)
    rhs_v, lower_v, upper_v, diag_v, counts_v, basis_v = take(6)
    gathered = take(levels - 1)
    outgoing = take(levels - 1)
    incoming = take(levels - 1)
    (pattern_s,) = take(1)
    spread = take(levels - 1)
    (totals,) = take(1)
    load_sem, fwd_send, fwd_recv, bwd_send, bwd_recv, sum_send, sum_recv = take(7)
    near_sem, far_sem = take(2)

    leaf = lax.axis_index("leaf")
    tile = lax.axis_index("tile")
    me = leaf * n_tile + tile

    def load(number, source, target):
        copy = pltpu.make_async_copy(source, target, load_sem.at[number])
        copy.start()
        return copy

    rhs_load = load(0, rhs_any, rhs_v)
    pattern_load = load(1, pattern_any, pattern_s)
    counts_load = load(2, counts_any, counts_v)
    lower_load = [
        load(3 + k, lower_any.at[k], lower_v.at[k]) for k in range(levels - 1)
    ]
    diag_load = load(levels + 2, diag_any, diag_v)
    upper_load = load(levels + 3, upper_any, upper_v)
    basis_load = load(levels + 4, basis_any, basis_v)

    def each_peer(leaves, visit):
        first = lax.div(leaf, leaves) * leaves
        own = leaf - first
        others = [(tile + step) % n_tile if step else tile for step in range(n_tile)]

        def far(step, carry):
            near = lax.rem(own + step, leaves)
            for other in others:
                visit(first + near, other, near * n_tile + other)
            return carry

        if leaves <= 16:
            for step in range(leaves // 2, leaves):
                far(step, 0)
            for step in range(1, leaves // 2):
                far(step, 0)
        else:
            lax.fori_loop(1, leaves, far, 0)
        for other in others[1:]:
            visit(leaf, other, own * n_tile + other)

    barrier = pltpu.get_barrier_semaphore()
    beside = lax.div(leaf, 2) * 2 + lax.rem(leaf + 1, 2)

    def greet(semaphore, to_leaf, to_tile):
        pl.semaphore_signal(
            semaphore, inc=1, device_id=(to_leaf, to_tile), device_id_type=MESH
        )

    greet(barrier, beside, 0)

    @pl.when(tile == 0)
    def _():
        pl.semaphore_wait(barrier, 3)
        greet(near_sem, leaf, 1)

    @pl.when(tile == 1)
    def _():
        greet(barrier, leaf, 0)
        pl.semaphore_wait(near_sem, 1)

        def far(step, carry):
            greet(barrier, lax.rem(leaf + step, n_leaf), 1)
            return carry

        if n_leaf <= 16:
            for step in range(1, n_leaf):
                far(step, 0)
        else:
            lax.fori_loop(1, n_leaf, far, 0)

    def everyone_entered():
        @pl.when(tile == 1)
        def _():
            pl.semaphore_wait(barrier, n_leaf - 1)
            greet(far_sem, leaf, 0)

        @pl.when(tile == 0)
        def _():
            pl.semaphore_wait(far_sem, 1)

    rhs_load.wait()
    counts_load.wait()
    live = [
        [
            (counts_v[0:1, k : k + 1] > t).astype(jnp.float32)
            for t in range(tiles)
        ]
        for k in range(levels)
    ]

    def source(k, t, n):
        return pattern_s[n, k, me * tiles + t]

    def selectors(k):
        span = gathered[k].shape[0]
        lane_pair, lane_column = split(
            lax.broadcasted_iota(jnp.int32, (1, pairs * columns), 1), columns
        )
        wanted = jnp.zeros((1, pairs * columns), jnp.int32)
        for t in range(tiles):
            for n in range(neighbours):
                wanted = jnp.where(lane_pair == t * neighbours + n, source(k, t, n), wanted)
        row_tile, row_column = split(
            lax.broadcasted_iota(jnp.int32, (span * width, pairs * columns), 0), columns
        )
        chosen = (row_tile == wanted) & (row_column == lane_column)
        spread[k][...] = jnp.where(chosen, 1.0, 0.0).astype(jnp.bfloat16)

    def group(k):
        span = gathered[k].shape[0]
        return span, lax.rem(me, span)

    def arrived(buffer, semaphore, span):
        part = buffer.at[pl.ds(0, span - 1)]
        pltpu.make_async_copy(part, part, semaphore).wait()

    forward_vals = [[live[0][t] * rhs_v[0, t] for t in range(tiles)]]
    for k in range(1, levels):
        buffer = gathered[k - 1]
        span, slot = group(k - 1)
        buffer[slot] = jnp.concatenate(forward_vals[-1], 0).astype(jnp.bfloat16)
        if k == 2:
            everyone_entered()

        def send(to_leaf, to_tile, index):
            pltpu.make_async_remote_copy(
                src_ref=buffer.at[slot],
                dst_ref=buffer.at[slot],
                send_sem=fwd_send.at[k - 1],
                recv_sem=fwd_recv.at[k - 1],
                device_id=(to_leaf, to_tile),
                device_id_type=MESH,
            ).start()

        each_peer(span // n_tile, send)
        if k == 1:
            pattern_load.wait()
        selectors(k - 1)
        lower_load[k - 1].wait()
        arrived(buffer, fwd_recv.at[k - 1], span)
        picked = []
        for t in range(tiles):
            for n in range(neighbours):
                owner, place = split(source(k - 1, t, n), tiles)
                both = buffer[owner].astype(jnp.float32)
                chosen = both[:columns]
                for other in range(1, tiles):
                    part = both[other * columns : (other + 1) * columns]
                    chosen = jnp.where(place == other, part, chosen)
                picked.append(chosen.astype(jnp.bfloat16))
        values = []
        for t in range(tiles):
            coupling = None
            for n in range(neighbours):
                q = t * neighbours + n
                term = lax.dot_general(
                    picked[q],
                    lower_v[k - 1, t, n],
                    NT,
                    preferred_element_type=jnp.float32,
                )
                coupling = term if coupling is None else coupling + term
            values.append(live[k][t] * (rhs_v[k, t] - coupling))
        forward_vals.append(values)

    diag_load.wait()
    upper_load.wait()
    basis_load.wait()
    partial = [None] * basis_size
    squares = None

    def project(k, values):
        nonlocal squares
        for t in range(tiles):
            for m in range(basis_size):
                term = basis_v[m, k, t] * values[t]
                partial[m] = term if partial[m] is None else partial[m] + term
            term = values[t] * values[t]
            squares = term if squares is None else squares + term

    upstream = None
    for k in reversed(range(levels)):
        values = []
        for t in range(tiles):
            operand = forward_vals[k][t]
            if upstream is not None:
                operand = operand - upstream[t * columns : (t + 1) * columns]
            value = live[k][t] * lax.dot_general(
                operand.astype(jnp.bfloat16),
                diag_v[k, t],
                NT,
                preferred_element_type=jnp.float32,
            )
            precond_ref[k, t] = value
            values.append(value)
        if k > 0:
            span, slot = group(k - 1)
            products = []
            for t in range(tiles):
                rounded = values[t].astype(jnp.bfloat16)
                for n in range(neighbours):
                    products.append(
                        lax.dot_general(
                            rounded,
                            upper_v[k - 1, t, n],
                            NT,
                            preferred_element_type=jnp.float32,
                        )
                    )
            products = jnp.concatenate(products, 0).astype(jnp.bfloat16)
            out, into = outgoing[k - 1], incoming[k - 1]
            out[...] = (
                jnp.dot(spread[k - 1][...], products, preferred_element_type=jnp.float32)
                .astype(jnp.bfloat16)
                .reshape(span, width, rows)
            )

            def send(to_leaf, to_tile, index):
                pltpu.make_async_remote_copy(
                    src_ref=out.at[index],
                    dst_ref=into.at[slot],
                    send_sem=bwd_send.at[k - 1],
                    recv_sem=bwd_recv.at[k - 1],
                    device_id=(to_leaf, to_tile),
                    device_id_type=MESH,
                ).start()

            each_peer(span // n_tile, send)
            into[slot] = out[slot]
            project(k, values)
            arrived(into, bwd_recv.at[k - 1], span)
            upstream = jnp.sum(into[...].astype(jnp.float32), axis=0)
        else:
            project(k, values)

    lane = lax.broadcasted_iota(jnp.int32, (columns, rows), 1)
    seat = lane - lax.broadcasted_iota(jnp.int32, (columns, rows), 0)
    packed = jnp.zeros((columns, rows), jnp.float32)
    for m, term in enumerate(partial + [squares]):
        reduced = jnp.sum(term, axis=1, keepdims=True)
        packed = jnp.where(seat == m * columns, reduced, packed)
    totals[me] = jnp.sum(packed, axis=0, keepdims=True)

    def send(to_leaf, to_tile, index):
        pltpu.make_async_remote_copy(
            src_ref=totals.at[me],
            dst_ref=totals.at[me],
            send_sem=sum_send,
            recv_sem=sum_recv,
            device_id=(to_leaf, to_tile),
            device_id_type=MESH,
        ).start()

    each_peer(n_leaf, send)
    for k in range(1, levels):
        span, slot = group(k - 1)
        arrived(gathered[k - 1], fwd_send.at[k - 1], span)
        arrived(outgoing[k - 1], bwd_send.at[k - 1], span)
    arrived(totals, sum_recv, devices)
    summed = jnp.broadcast_to(jnp.sum(totals[...], axis=0), (columns, rows))
    spaced = jnp.where(split(lane, columns)[1] == lane - seat, summed, 0.0)
    row_block, _ = split(lax.broadcasted_iota(jnp.int32, (rows, rows), 0), columns)
    compress = row_block == lax.broadcasted_iota(jnp.int32, (rows, rows), 1)
    total = jnp.dot(
        spaced,
        jnp.where(compress, 1.0, 0.0),
        precision=lax.Precision.HIGHEST,
        preferred_element_type=jnp.float32,
    )
    squared = jnp.sum(jnp.where(lane == basis_size, total, 0.0), axis=1, keepdims=True)
    explained = jnp.sum(
        jnp.where(lane < basis_size, total * total, 0.0), axis=1, keepdims=True
    )
    norm = jnp.sqrt(jnp.maximum(squared - explained, 0.0) + epsilon)
    scaled = norm / math.sqrt(levels * tiles * rows * devices)
    result = jnp.where(lane == basis_size, scaled, total)
    coeffs_ref[...] = result[:, : basis_size + 1]
    arrived(totals, sum_send, devices)


def local(rhs, lower, upper, diag_inv, pattern, counts, basis):
    levels, tiles, columns, rows = rhs.shape
    neighbours = lower.shape[2]
    basis_size = basis.shape[0]
    n_leaf, n_tile = lax.axis_size("leaf"), lax.axis_size("tile")
    dims = (levels, tiles, columns, rows, neighbours, basis_size, n_leaf, n_tile)
    spans = [2 ** (k + 1) for k in range(1, levels)]
    width, pairs = tiles * columns, tiles * neighbours
    pattern, counts = jnp.transpose(pattern, (2, 0, 1)), counts.T
    operands = (rhs, lower, upper, diag_inv, pattern, counts, basis)
    slots = [pltpu.VMEM((span, width, rows), jnp.bfloat16) for span in spans]
    scratch = [
        pltpu.VMEM(operand.shape, operand.dtype) for operand in operands if operand is not pattern
    ]
    scratch += slots * 3
    scratch += [pltpu.SMEM(pattern.shape, pattern.dtype)]
    scratch += [pltpu.VMEM((span * width, pairs * columns), jnp.bfloat16) for span in spans]
    scratch += [pltpu.VMEM((n_leaf * n_tile, 1, rows), jnp.float32)]
    scratch += [pltpu.SemaphoreType.DMA((levels + 5,))]
    scratch += [pltpu.SemaphoreType.DMA((levels - 1,))] * 4
    scratch += [pltpu.SemaphoreType.DMA] * 2
    scratch += [pltpu.SemaphoreType.REGULAR] * 2
    precond, coeffs = pl.pallas_call(
        functools.partial(kernel, dims),
        name="sweep",
        out_shape=(
            jax.ShapeDtypeStruct(rhs.shape, jnp.float32),
            jax.ShapeDtypeStruct((columns, basis_size + 1), jnp.float32),
        ),
        in_specs=[pl.BlockSpec(memory_space=pl.ANY)] * len(operands),
        out_specs=[pl.BlockSpec(memory_space=pltpu.VMEM)] * 2,
        scratch_shapes=scratch,
        compiler_params=pltpu.CompilerParams(collective_id=0, has_side_effects=True),
    )(*operands)
    return precond, coeffs.T


def solution(mesh):
    return jax.shard_map(
        local,
        mesh=mesh,
        in_specs=(
            P(None, ("leaf", "tile"), None, None),
            P(None, ("leaf", "tile"), None, None, None),
            P(None, ("leaf", "tile"), None, None, None),
            P(None, ("leaf", "tile"), None, None),
            P(),
            P(None, ("leaf", "tile")),
            P(None, None, ("leaf", "tile"), None, None),
        ),
        out_specs=(P(None, ("leaf", "tile"), None, None), P()),
        check_vma=False,
    )
```

```python
import functools
import math

import jax
import jax.numpy as jnp
from jax import lax
from jax.experimental import pallas as pl
from jax.experimental.pallas import tpu as pltpu
from jax.sharding import PartitionSpec as P

epsilon = 1e-06
MESH = pl.DeviceIdType.MESH
NT = (((1,), (1,)), ((), ()))


def split(index, size):
    if size & (size - 1) == 0:
        return lax.shift_right_logical(index, size.bit_length() - 1), index & (size - 1)
    return index // size, index % size


def kernel(dims, *refs):
    levels, tiles, columns, rows, neighbours, basis_size, n_leaf, n_tile = dims
    devices = n_leaf * n_tile
    width = tiles * columns
    pairs = tiles * neighbours
    refs = list(refs)

    def take(count):
        taken = refs[:count]
        del refs[:count]
        return taken

    rhs_any, lower_any, upper_any, diag_any, pattern_any, counts_any, basis_any = take(7)
    precond_ref, coeffs_ref = take(2)
    rhs_v, lower_v, upper_v, diag_v, counts_v, basis_v = take(6)
    gathered = take(levels - 1)
    outgoing = take(levels - 1)
    incoming = take(levels - 1)
    (pattern_s,) = take(1)
    spread = take(levels - 1)
    (totals,) = take(1)
    load_sem, fwd_send, fwd_recv, bwd_send, bwd_recv, sum_send, sum_recv = take(7)
    near_sem, sibling_sem, far_sem = take(3)

    leaf = lax.axis_index("leaf")
    tile = lax.axis_index("tile")
    me = leaf * n_tile + tile

    def load(number, source, target):
        copy = pltpu.make_async_copy(source, target, load_sem.at[number])
        copy.start()
        return copy

    rhs_load = load(0, rhs_any, rhs_v)
    pattern_load = load(1, pattern_any, pattern_s)
    counts_load = load(2, counts_any, counts_v)
    lower_load = [
        load(3 + k, lower_any.at[k], lower_v.at[k]) for k in range(levels - 1)
    ]
    diag_load = load(levels + 2, diag_any, diag_v)
    upper_load = load(levels + 3, upper_any, upper_v)
    basis_load = load(levels + 4, basis_any, basis_v)

    def each_peer(leaves, visit):
        first = lax.div(leaf, leaves) * leaves
        own = leaf - first
        others = [(tile + step) % n_tile if step else tile for step in range(n_tile)]

        def far(step, carry):
            near = lax.rem(own + step, leaves)
            for other in others:
                visit(first + near, other, near * n_tile + other)
            return carry

        if leaves <= 16:
            for step in range(leaves // 2, leaves):
                far(step, 0)
            for step in range(1, leaves // 2):
                far(step, 0)
        else:
            lax.fori_loop(1, leaves, far, 0)
        for other in others[1:]:
            visit(leaf, other, own * n_tile + other)

    barrier = pltpu.get_barrier_semaphore()
    pair, odd = lax.div(leaf, 2), lax.rem(leaf, 2)
    pair_count = n_leaf // 2
    beside = pair * 2 + (1 - odd)
    meets_sibling = (tile == 1) & (odd == 0)
    meets_all = (tile == 1) & (odd == 1)

    def greet(semaphore, to_leaf, to_tile):
        pl.semaphore_signal(
            semaphore, inc=1, device_id=(to_leaf, to_tile), device_id_type=MESH
        )

    greet(barrier, beside, 0)

    @pl.when(tile == 0)
    def _():
        pl.semaphore_wait(barrier, 3)
        greet(near_sem, leaf, 1)

    @pl.when(tile == 1)
    def _():
        greet(barrier, leaf, 0)
        pl.semaphore_wait(near_sem, 1)

    @pl.when(meets_sibling)
    def _():
        greet(barrier, (lax.div(pair, 2) * 2 + 1 - lax.rem(pair, 2)) * 2, 1)

    @pl.when(meets_all)
    def _():
        def far(step, carry):
            greet(barrier, lax.rem(pair + step, pair_count) * 2 + 1, 1)
            return carry

        if pair_count <= 16:
            for step in range(1, pair_count):
                far(step, 0)
        else:
            lax.fori_loop(1, pair_count, far, 0)

    def relay(heard, count, semaphore):
        @pl.when(heard)
        def _():
            pl.semaphore_wait(barrier, count)
            greet(semaphore, beside, 0)
            greet(semaphore, beside, 1)
            greet(semaphore, leaf, 0)

    def learn(heard, semaphore):
        @pl.when(jnp.logical_not(heard))
        def _():
            pl.semaphore_wait(semaphore, 1)

    rhs_load.wait()
    counts_load.wait()
    live = [
        [
            (counts_v[0:1, k : k + 1] > t).astype(jnp.float32)
            for t in range(tiles)
        ]
        for k in range(levels)
    ]

    def source(k, t, n):
        return pattern_s[n, k, me * tiles + t]

    def selectors(k):
        span = gathered[k].shape[0]
        lane_pair, lane_column = split(
            lax.broadcasted_iota(jnp.int32, (1, pairs * columns), 1), columns
        )
        wanted = jnp.zeros((1, pairs * columns), jnp.int32)
        for t in range(tiles):
            for n in range(neighbours):
                wanted = jnp.where(lane_pair == t * neighbours + n, source(k, t, n), wanted)
        row_tile, row_column = split(
            lax.broadcasted_iota(jnp.int32, (span * width, pairs * columns), 0), columns
        )
        chosen = (row_tile == wanted) & (row_column == lane_column)
        spread[k][...] = jnp.where(chosen, 1.0, 0.0).astype(jnp.bfloat16)

    def group(k):
        span = gathered[k].shape[0]
        return span, lax.rem(me, span)

    def arrived(buffer, semaphore, span):
        part = buffer.at[pl.ds(0, span - 1)]
        pltpu.make_async_copy(part, part, semaphore).wait()

    forward_vals = [[live[0][t] * rhs_v[0, t] for t in range(tiles)]]
    for k in range(1, levels):
        buffer = gathered[k - 1]
        span, slot = group(k - 1)
        buffer[slot] = jnp.concatenate(forward_vals[-1], 0).astype(jnp.bfloat16)
        if k == 2:
            learn(meets_sibling, sibling_sem)
        if k == 3:
            learn(meets_all, far_sem)

        def send(to_leaf, to_tile, index):
            pltpu.make_async_remote_copy(
                src_ref=buffer.at[slot],
                dst_ref=buffer.at[slot],
                send_sem=fwd_send.at[k - 1],
                recv_sem=fwd_recv.at[k - 1],
                device_id=(to_leaf, to_tile),
                device_id_type=MESH,
            ).start()

        each_peer(span // n_tile, send)
        if k == 1:
            pattern_load.wait()
        selectors(k - 1)
        if k == 1:
            relay(meets_sibling, 1, sibling_sem)
        if k == 2:
            relay(meets_all, pair_count - 1, far_sem)
        lower_load[k - 1].wait()
        arrived(buffer, fwd_recv.at[k - 1], span)
        picked = []
        for t in range(tiles):
            for n in range(neighbours):
                owner, place = split(source(k - 1, t, n), tiles)
                both = buffer[owner].astype(jnp.float32)
                chosen = both[:columns]
                for other in range(1, tiles):
                    part = both[other * columns : (other + 1) * columns]
                    chosen = jnp.where(place == other, part, chosen)
                picked.append(chosen.astype(jnp.bfloat16))
        values = []
        for t in range(tiles):
            coupling = None
            for n in range(neighbours):
                q = t * neighbours + n
                term = lax.dot_general(
                    picked[q],
                    lower_v[k - 1, t, n],
                    NT,
                    preferred_element_type=jnp.float32,
                )
                coupling = term if coupling is None else coupling + term
            values.append(live[k][t] * (rhs_v[k, t] - coupling))
        forward_vals.append(values)

    diag_load.wait()
    upper_load.wait()
    basis_load.wait()
    partial = [None] * basis_size
    squares = None

    def project(k, values):
        nonlocal squares
        for t in range(tiles):
            for m in range(basis_size):
                term = basis_v[m, k, t] * values[t]
                partial[m] = term if partial[m] is None else partial[m] + term
            term = values[t] * values[t]
            squares = term if squares is None else squares + term

    upstream = None
    for k in reversed(range(levels)):
        values = []
        for t in range(tiles):
            operand = forward_vals[k][t]
            if upstream is not None:
                operand = operand - upstream[t * columns : (t + 1) * columns]
            value = live[k][t] * lax.dot_general(
                operand.astype(jnp.bfloat16),
                diag_v[k, t],
                NT,
                preferred_element_type=jnp.float32,
            )
            precond_ref[k, t] = value
            values.append(value)
        if k > 0:
            span, slot = group(k - 1)
            products = []
            for t in range(tiles):
                rounded = values[t].astype(jnp.bfloat16)
                for n in range(neighbours):
                    products.append(
                        lax.dot_general(
                            rounded,
                            upper_v[k - 1, t, n],
                            NT,
                            preferred_element_type=jnp.float32,
                        )
                    )
            products = jnp.concatenate(products, 0).astype(jnp.bfloat16)
            out, into = outgoing[k - 1], incoming[k - 1]
            out[...] = (
                jnp.dot(spread[k - 1][...], products, preferred_element_type=jnp.float32)
                .astype(jnp.bfloat16)
                .reshape(span, width, rows)
            )

            def send(to_leaf, to_tile, index):
                pltpu.make_async_remote_copy(
                    src_ref=out.at[index],
                    dst_ref=into.at[slot],
                    send_sem=bwd_send.at[k - 1],
                    recv_sem=bwd_recv.at[k - 1],
                    device_id=(to_leaf, to_tile),
                    device_id_type=MESH,
                ).start()

            each_peer(span // n_tile, send)
            into[slot] = out[slot]
            project(k, values)
            arrived(into, bwd_recv.at[k - 1], span)
            upstream = jnp.sum(into[...].astype(jnp.float32), axis=0)
        else:
            project(k, values)

    lane = lax.broadcasted_iota(jnp.int32, (columns, rows), 1)
    seat = lane - lax.broadcasted_iota(jnp.int32, (columns, rows), 0)
    packed = jnp.zeros((columns, rows), jnp.float32)
    for m, term in enumerate(partial + [squares]):
        reduced = jnp.sum(term, axis=1, keepdims=True)
        packed = jnp.where(seat == m * columns, reduced, packed)
    totals[me] = jnp.sum(packed, axis=0, keepdims=True)

    def send(to_leaf, to_tile, index):
        pltpu.make_async_remote_copy(
            src_ref=totals.at[me],
            dst_ref=totals.at[me],
            send_sem=sum_send,
            recv_sem=sum_recv,
            device_id=(to_leaf, to_tile),
            device_id_type=MESH,
        ).start()

    each_peer(n_leaf, send)
    for k in range(1, levels):
        span, slot = group(k - 1)
        arrived(gathered[k - 1], fwd_send.at[k - 1], span)
        arrived(outgoing[k - 1], bwd_send.at[k - 1], span)
    arrived(totals, sum_recv, devices)
    summed = jnp.broadcast_to(jnp.sum(totals[...], axis=0), (columns, rows))
    spaced = jnp.where(split(lane, columns)[1] == lane - seat, summed, 0.0)
    row_block, _ = split(lax.broadcasted_iota(jnp.int32, (rows, rows), 0), columns)
    compress = row_block == lax.broadcasted_iota(jnp.int32, (rows, rows), 1)
    total = jnp.dot(
        spaced,
        jnp.where(compress, 1.0, 0.0),
        precision=lax.Precision.HIGHEST,
        preferred_element_type=jnp.float32,
    )
    squared = jnp.sum(jnp.where(lane == basis_size, total, 0.0), axis=1, keepdims=True)
    explained = jnp.sum(
        jnp.where(lane < basis_size, total * total, 0.0), axis=1, keepdims=True
    )
    norm = jnp.sqrt(jnp.maximum(squared - explained, 0.0) + epsilon)
    scaled = norm / math.sqrt(levels * tiles * rows * devices)
    result = jnp.where(lane == basis_size, scaled, total)
    coeffs_ref[...] = result[:, : basis_size + 1]
    arrived(totals, sum_send, devices)


def local(rhs, lower, upper, diag_inv, pattern, counts, basis):
    levels, tiles, columns, rows = rhs.shape
    neighbours = lower.shape[2]
    basis_size = basis.shape[0]
    n_leaf, n_tile = lax.axis_size("leaf"), lax.axis_size("tile")
    dims = (levels, tiles, columns, rows, neighbours, basis_size, n_leaf, n_tile)
    spans = [2 ** (k + 1) for k in range(1, levels)]
    width, pairs = tiles * columns, tiles * neighbours
    pattern, counts = jnp.transpose(pattern, (2, 0, 1)), counts.T
    operands = (rhs, lower, upper, diag_inv, pattern, counts, basis)
    slots = [pltpu.VMEM((span, width, rows), jnp.bfloat16) for span in spans]
    scratch = [
        pltpu.VMEM(operand.shape, operand.dtype) for operand in operands if operand is not pattern
    ]
    scratch += slots * 3
    scratch += [pltpu.SMEM(pattern.shape, pattern.dtype)]
    scratch += [pltpu.VMEM((span * width, pairs * columns), jnp.bfloat16) for span in spans]
    scratch += [pltpu.VMEM((n_leaf * n_tile, 1, rows), jnp.float32)]
    scratch += [pltpu.SemaphoreType.DMA((levels + 5,))]
    scratch += [pltpu.SemaphoreType.DMA((levels - 1,))] * 4
    scratch += [pltpu.SemaphoreType.DMA] * 2
    scratch += [pltpu.SemaphoreType.REGULAR] * 3
    precond, coeffs = pl.pallas_call(
        functools.partial(kernel, dims),
        name="sweep",
        out_shape=(
            jax.ShapeDtypeStruct(rhs.shape, jnp.float32),
            jax.ShapeDtypeStruct((columns, basis_size + 1), jnp.float32),
        ),
        in_specs=[pl.BlockSpec(memory_space=pl.ANY)] * len(operands),
        out_specs=[pl.BlockSpec(memory_space=pltpu.VMEM)] * 2,
        scratch_shapes=scratch,
        compiler_params=pltpu.CompilerParams(collective_id=0, has_side_effects=True),
    )(*operands)
    return precond, coeffs.T


def solution(mesh):
    return jax.shard_map(
        local,
        mesh=mesh,
        in_specs=(
            P(None, ("leaf", "tile"), None, None),
            P(None, ("leaf", "tile"), None, None, None),
            P(None, ("leaf", "tile"), None, None, None),
            P(None, ("leaf", "tile"), None, None),
            P(),
            P(None, ("leaf", "tile")),
            P(None, None, ("leaf", "tile"), None, None),
        ),
        out_specs=(P(None, ("leaf", "tile"), None, None), P()),
        check_vma=False,
    )
```
